32 devices in a mesh: query: 4 (over y, x), train: 4 (over z), mp: 2 (over core).
Axes of the slice: x: 2, y: 2, z: 4, core: 2. Of those that a mesh axis runs over, the one named last changes fastest.
Arguments:
- residual: bfloat16 [512, 8192], P('train'), may hold values from -6 to 6
- norm_gain: float32 [8192], replicated, may hold values from 0.1 to 1.9
- gate_weight: bfloat16 [8192, 14336], P('train', ('query', 'mp')), may hold values from -0.0625 to 0.0625
- up_weight: bfloat16 [8192, 14336], P('train', ('query', 'mp')), may hold values from -0.0625 to 0.0625
- out_grad: bfloat16 [512, 8192], P('train', ('query', 'mp')), may hold values from -6 to 6
- left_factor: bfloat16 [8, 32, 14336], P(('query', 'mp')), may hold values from -0.0078125 to 0.0078125
- right_factor: bfloat16 [8, 32, 8192], P(('query', 'mp')), may hold values from -0.0625 to 0.0625
Outputs:
- scores: float32 [8, 512], P(('query', 'mp'), 'train')
The draws below stay inside these ranges and needn't reach their ends.
All inputs are finite; a program needn't handle non-finite values.
Results may differ from the reference program's by a relative error of at most 0.023.
Values may be sent and summed in bfloat16 or wider, within the bound.
A program may use at most 64 MiB of HBM per device.

```python
import jax
import jax.numpy as jnp
from jax import lax

D = 8192
FF = 14336
R = 32
TOKENS = 512
NQ = 8
N_TRAIN = 4


def level_of(rng, shape, cuts, least, top_value):
    gain, own = 1.0, jax.random.fold_in(rng, 6)
    for dim, shards_of in cuts:
        draws = jnp.exp(jax.random.uniform(jax.random.fold_in(own, dim), (shards_of,), jnp.float32, least / len(cuts), top_value / len(cuts)))
        gain = gain * jnp.repeat(draws, shape[dim] // shards_of).reshape([-1 if axis == dim else 1 for axis in range(len(shape))])
    return gain


def gaussian(stream_key, shape, deviation, bound, cuts=(), held_as=jnp.bfloat16):
    values = jax.random.normal(stream_key, shape, jnp.float32) * deviation
    if len(cuts) > 0:
        values = level_of(stream_key, shape, cuts, -0.22, 0.18) * values
    return jnp.clip(values, min=-bound, max=bound).astype(held_as)


def setup_inputs(seed: int = 0) -> dict:
    streams_of = jax.random.split(jax.random.key(seed), 8)
    return {
        "residual": gaussian(streams_of[0], (TOKENS, D), 1.0, 6.0, ((0, 4),)),
        "norm_gain": jnp.clip(1.0 + 0.18 * jax.random.normal(streams_of[1], (D,), jnp.float32), 0.1, 1.9),
        "gate_weight": gaussian(streams_of[2], (D, FF), D ** -0.5, 0.0625, ((0, 4), (1, 8))),
        "up_weight": gaussian(streams_of[3], (D, FF), D ** -0.5, 0.0625, ((0, 4), (1, 8))),
        "out_grad": gaussian(streams_of[4], (TOKENS, D), 1.0, 6.0, ((0, 4), (1, 8))),
        "left_factor": gaussian(streams_of[5], (NQ, R, FF), (FF * R) ** -0.5, 0.0078125, ((0, 8),)),
        "right_factor": gaussian(streams_of[6], (NQ, R, D), D ** -0.5, 0.0625, ((0, 8),)),
    }


norm_eps = 1e-05

def reference(residual, norm_gain, gate_weight, up_weight, out_grad, left_factor, right_factor):
    values = residual.astype(jnp.float32)
    mean_sq = lax.optimization_barrier(jnp.mean(values * values, axis=1, keepdims=True))
    normed = (values * lax.rsqrt(mean_sq + norm_eps) * norm_gain[None, :]).astype(jnp.bfloat16)
    block_rows = D // N_TRAIN
    normed_blocks = normed.reshape(TOKENS, N_TRAIN, block_rows).transpose(1, 0, 2)
    paired = jnp.concatenate([gate_weight, up_weight], axis=1).reshape(N_TRAIN, block_rows, 2 * FF)

    def add_block(running, pieces):
        row_block, weight_block = pieces
        term = jnp.dot(row_block, weight_block, preferred_element_type=jnp.float32).astype(jnp.bfloat16)
        term = lax.optimization_barrier(term).astype(jnp.float32)
        return (running + term, None)
    summed, unused = lax.scan(add_block, jnp.zeros((TOKENS, 2 * FF), jnp.float32), (normed_blocks, paired))
    activation = (jax.nn.silu(summed[:, :FF]) * summed[:, FF:]).astype(jnp.bfloat16)
    contract = (((1,), (1,)), ((), ()))
    projected = lax.dot_general(left_factor.reshape(NQ * R, FF), activation, contract, preferred_element_type=jnp.float32)
    sensed = lax.dot_general(right_factor.reshape(NQ * R, D), out_grad, contract, preferred_element_type=jnp.float32)
    return lax.optimization_barrier(jnp.sum((projected * sensed).reshape(NQ, R, TOKENS), axis=1))
```

```python
import functools

import jax
import jax.numpy as jnp
from jax import lax
from jax.experimental import pallas as pl
from jax.experimental.pallas import tpu as pltpu
from jax.sharding import PartitionSpec as P

norm_eps = 1e-05


def on_device(residual, norm_gain, gate_weight, up_weight, out_grad, left_factor, right_factor):
    values = residual.astype(jnp.float32)
    mean_sq = jnp.mean(values * values, axis=1, keepdims=True)
    normed = (values * lax.rsqrt(mean_sq + norm_eps) * norm_gain[None, :]).astype(jnp.bfloat16)
    tok_rows = normed.shape[0]
    hidden_cols = gate_weight.shape[1]
    all_rows = lax.all_to_all(normed, "train", split_axis=1, concat_axis=0, tiled=True)
    paired = jnp.concatenate([gate_weight, up_weight], axis=1)
    summed = lax.psum_scatter(
        jnp.dot(all_rows, paired, preferred_element_type=jnp.float32).astype(jnp.bfloat16),
        "train",
        scatter_dimension=0,
        tiled=True,
    ).astype(jnp.float32)
    activation = (jax.nn.silu(summed[:, :hidden_cols]) * summed[:, hidden_cols:]).astype(
        jnp.bfloat16
    )
    queries = left_factor.shape[0]
    factor_rank = left_factor.shape[1]
    contract = (((1,), (1,)), ((), ()))
    left_flat = left_factor.reshape(queries * factor_rank, left_factor.shape[2])
    columns = left_flat
    projected = lax.dot_general(
        columns,
        lax.all_gather(activation, ("query", "mp"), axis=1, tiled=True),
        contract,
        preferred_element_type=jnp.float32,
    )
    right_flat = right_factor.reshape(queries * factor_rank, right_factor.shape[2])
    columns = right_flat
    sensed = lax.dot_general(
        columns,
        lax.all_gather(out_grad, ("query", "mp"), axis=1, tiled=True),
        contract,
        preferred_element_type=jnp.float32,
    )
    return jnp.sum((projected * sensed).reshape(queries, factor_rank, tok_rows), axis=1)


LANES = 128
SUBLANES = 16
LAG = 2
MESH = pl.DeviceIdType.MESH
NT = (((1,), (1,)), ((), ()))


def remote(src, dst, send_sem, recv_sem, device):
    return pltpu.make_async_remote_copy(
        src_ref=src,
        dst_ref=dst,
        send_sem=send_sem,
        recv_sem=recv_sem,
        device_id=device,
        device_id_type=MESH,
    )


def kernel(
    n, nq, nm,
    residual, gain, gate, up, grad, left, right,
    out,
    raw, x, w, own, gain_v, stat_own, stat, part, from_up, from_down, lf, rf, grad_v, act,
    sens_part, sens_in, proj_part, proj_in,
    ld_sem, w_sem, x_send, x_recv, f_send, f_recv, sib_send, sib_recv,
    l_send, l_recv, r_send, r_recv, s_send, s_recv, p_send, p_recv, t_send, t_recv,
    dn_send, dn_recv, up_send, up_recv,
):
    q, z, m = lax.axis_index("query"), lax.axis_index("train"), lax.axis_index("mp")
    planes = nq * nm
    p = q * nm + m
    rows = residual.shape[0]
    depth = gate.shape[0]
    cols = gate.shape[1]
    width = grad.shape[1]
    rank = left.shape[0]
    chunks = cols // LANES
    part_rows = rows // planes
    half = n // 2
    side = half * rows
    low = z < half
    end = jnp.where(low, 0, n - 1)
    slot = z - jnp.where(low, 0, half)
    is_end = jnp.logical_or(z == 0, z == n - 1)

    def dev(qq, zz, mm):
        return {"query": qq, "train": zz, "mp": mm}

    sibling = dev(q, z, 1 - m)

    def piece(zz, qq, mm):
        start = zz * rows + (qq * nm + mm) * part_rows
        return raw.at[pl.ds(pl.multiple_of(start, part_rows), part_rows), :]

    def around(d):
        return lax.rem(z + d, n)

    def x_copy(d):
        zt = around(d)
        return remote(
            residual.at[
                pl.ds(pl.multiple_of(p * part_rows, part_rows), part_rows),
                pl.ds(pl.multiple_of(zt * depth, depth), depth),
            ],
            piece(z, q, m), x_send.at[d], x_recv.at[z], dev(q, zt, m),
        )

    for d in range(1, n):
        x_copy(d).start()
    own_x = pltpu.make_async_copy(
        residual.at[:, pl.ds(pl.multiple_of(z * depth, depth), depth)],
        raw.at[pl.ds(pl.multiple_of(z * rows, rows), rows), :], ld_sem.at[0])
    own_all = pltpu.make_async_copy(residual, own, ld_sem.at[1])
    gain_copy = pltpu.make_async_copy(gain, gain_v, ld_sem.at[2])
    grad_copy = pltpu.make_async_copy(grad, grad_v, ld_sem.at[3])

    def slice_of(factor, span, to):
        return factor.at[:, pl.ds(pl.multiple_of(to * span, LANES), span)]

    def rows_of(ref, who):
        return ref.at[pl.ds(pl.multiple_of(who * rank, rank), rank), :]

    own_l = pltpu.make_async_copy(slice_of(left, cols, p), rows_of(lf, p), ld_sem.at[4])
    own_r = pltpu.make_async_copy(slice_of(right, width, p), rows_of(rf, p), ld_sem.at[5])
    for copy in (own_all, own_x, gain_copy, grad_copy, own_l, own_r):
        copy.start()

    def w_copies(c):
        at = pl.ds(pl.multiple_of(c * LANES, LANES), LANES)
        return (
            pltpu.make_async_copy(gate.at[:, at], w.at[c, :, pl.ds(0, LANES)], w_sem.at[c, 0]),
            pltpu.make_async_copy(up.at[:, at], w.at[c, :, pl.ds(LANES, LANES)], w_sem.at[c, 1]),
        )

    @pl.loop(0, chunks)
    def _(c):
        for copy in w_copies(c):
            copy.start()

    own_all.wait()

    @pl.loop(0, rows // SUBLANES)
    def _(i):
        at = pl.ds(pl.multiple_of(i * SUBLANES, SUBLANES), SUBLANES)
        v = own[at, :].astype(jnp.float32)
        mean_sq = jnp.mean(v * v, axis=1, keepdims=True)
        stat_own[at, :] = jnp.broadcast_to(lax.rsqrt(mean_sq + norm_eps), (SUBLANES, LANES))

    def stat_rows(s):
        return pl.ds(pl.multiple_of(s * rows, rows), rows)

    stat_copy = remote(
        stat_own, stat.at[stat_rows(slot), :], t_send.at[0], t_recv.at[slot], dev(q, end, m))

    @pl.when(is_end)
    def _():
        stat[stat_rows(slot), :] = stat_own[...]

    @pl.when(jnp.logical_not(is_end))
    def _():
        stat_copy.start()

    def spread(d, dq):
        zs = around(d)
        if dq == 0:
            return remote(piece(zs, q, m), piece(zs, q, m), sib_send.at[d, 0], sib_recv.at[zs, q], sibling)
        return remote(
            piece(zs, q, m), piece(zs, q, m), f_send.at[d, dq], f_recv.at[zs, q],
            dev(lax.rem(q + dq, nq), z, m))

    def relay(d, dq):
        zs, qs = around(d), lax.rem(q + dq, nq)
        return remote(
            piece(zs, qs, m), piece(zs, qs, m), sib_send.at[d, dq], sib_recv.at[zs, qs], sibling)

    for d in range(1, n):
        zs = around(d)
        remote(piece(zs, q, m), piece(zs, q, m), x_send.at[d], x_recv.at[zs], sibling).wait_recv()
        for dq in range(nq):
            spread(d, (dq + 1) % nq).start()

    def factor_copies(k):
        to = lax.rem(p + k, planes)
        device = dev(to // nm, z, lax.rem(to, nm))
        return (
            remote(slice_of(right, width, to), rows_of(rf, p), r_send.at[k], r_recv.at[p], device),
            remote(slice_of(left, cols, to), rows_of(lf, p), l_send.at[k], l_recv.at[p], device),
        )

    for which in range(2):
        for k in range(1, planes):
            factor_copies(k)[which].start()
    for d in range(1, n):
        zs = around(d)
        for dq in range(1, nq):
            qs = lax.rem(q + dq, nq)
            remote(piece(zs, qs, m), piece(zs, qs, m), f_send.at[d, dq], f_recv.at[zs, qs], sibling).wait_recv()
            relay(d, dq).start()
    own_x.wait()
    gain_copy.wait()
    for d in range(1, n):
        zs = around(d)
        for dq in range(nq):
            qs = lax.rem(q + dq, nq)
            at = piece(zs, qs, 1 - m)
            remote(at, at, sib_send.at[d, dq], sib_recv.at[zs, qs], sibling).wait_recv()

    @pl.loop(0, n * rows // (4 * SUBLANES))
    def _(i):
        at = pl.ds(pl.multiple_of(i * 4 * SUBLANES, 4 * SUBLANES), 4 * SUBLANES)
        g = gain_v[:, pl.ds(pl.multiple_of(z * depth, depth), depth)]
        x[at, :] = (raw[at, :].astype(jnp.float32) * g).astype(jnp.bfloat16)

    down_rows, up_rows = pl.ds(0, side), pl.ds(side, side)

    def down_copy(c):
        return remote(
            part.at[c, down_rows, :], from_up.at[c], dn_send.at[c], dn_recv.at[c],
            dev(q, jnp.maximum(z - 1, 0), m))

    def up_copy(c):
        return remote(
            part.at[c, up_rows, :], from_down.at[c], up_send.at[c], up_recv.at[c],
            dev(q, jnp.minimum(z + 1, n - 1), m))

    for s in range(half):
        arrives = jnp.logical_and(is_end, slot != s)

        @pl.when(arrives)
        def _():
            remote(stat_own, stat.at[stat_rows(s), :], t_send.at[0], t_recv.at[s], sibling).wait_recv()

    def finish(c, total):
        s = stat[:, 0:1]
        g = total[:, :LANES] * s
        u = total[:, LANES:] * s
        act[:, pl.ds(pl.multiple_of(c * LANES, LANES), LANES)] = (
            g / (1.0 + jnp.exp(-g)) * u).astype(jnp.bfloat16)

    def pass_on(i, hops, arrived, copy, keep, last):
        c = i - LAG * hops

        @pl.when(jnp.logical_and(hops > 0, jnp.logical_and(c >= 0, c < chunks)))
        def _():
            copy(c).wait_recv()

            @pl.when(last)
            def _():
                finish(c, part[c, keep, :].astype(jnp.float32) + arrived[c].astype(jnp.float32))

            @pl.when(jnp.logical_not(last))
            def _():
                part[c, keep, :] = (
                    part[c, keep, :].astype(jnp.float32) + arrived[c].astype(jnp.float32)
                ).astype(jnp.bfloat16)
                copy(c).start()

    def sens_copy(k):
        to = lax.rem(p + k, planes)
        return remote(
            sens_part.at[to], sens_in.at[p], s_send.at[k], s_recv.at[p],
            dev(to // nm, z, lax.rem(to, nm)))

    def step(i, carry):
        @pl.when(i < chunks)
        def _():
            for copy in w_copies(i):
                copy.wait()
            part[i] = jnp.dot(x[...], w[i], preferred_element_type=jnp.float32).astype(jnp.bfloat16)

            @pl.when(z == n - 1)
            def _():
                down_copy(i).start()

            @pl.when(z == 0)
            def _():
                up_copy(i).start()

        pass_on(i, n - 1 - z, from_up, down_copy, down_rows, z == 0)
        pass_on(i, z, from_down, up_copy, up_rows, z == n - 1)

        @pl.when(i == chunks)
        def _():
            own_r.wait()
            grad_copy.wait()
            for k in range(1, planes):
                who = lax.rem(p + k, planes)
                at = rows_of(rf, who)
                remote(at, at, r_send.at[k], r_recv.at[who], sibling).wait_recv()
            sens_part[...] = lax.dot_general(
                rf[...], grad_v[...], NT, preferred_element_type=jnp.float32
            ).reshape(planes, rank, rows)
            sens_in[p] = sens_part[p]
            for k in range(1, planes):
                sens_copy(k).start()

        return carry

    lax.fori_loop(0, chunks + LAG * (n - 1), step, 0)

    own_l.wait()
    for k in range(1, planes):
        who = lax.rem(p + k, planes)
        at = rows_of(lf, who)
        remote(at, at, l_send.at[k], l_recv.at[who], sibling).wait_recv()

    def proj_copy(s, k):
        to = lax.rem(p + k, planes)
        return remote(
            proj_part.at[s, to], proj_in.at[p], p_send.at[s, k], p_recv.at[p],
            dev(to // nm, jnp.where(low, 0, half) + s, lax.rem(to, nm)))

    @pl.when(is_end)
    def _():
        product = lax.dot_general(lf[...], act[...], NT, preferred_element_type=jnp.float32)
        for s in range(half):
            proj_part[s] = product[:, s * rows:(s + 1) * rows].reshape(planes, rank, rows)
        for s in range(half):
            for k in range(planes):
                if k > 0:
                    proj_copy(s, k).start()
                else:
                    @pl.when(slot == s)
                    def _():
                        proj_in[p] = proj_part[s, p]

                    @pl.when(slot != s)
                    def _():
                        proj_copy(s, k).start()

    for k in range(1, planes):
        who = lax.rem(p + k, planes)
        remote(sens_part.at[0], sens_in.at[who], s_send.at[k], s_recv.at[who], sibling).wait_recv()
    for k in range(1, planes):
        who = lax.rem(p + k, planes)
        remote(proj_part.at[0, 0], proj_in.at[who], p_send.at[0, k], p_recv.at[who], sibling).wait_recv()

    @pl.when(jnp.logical_not(is_end))
    def _():
        remote(proj_part.at[0, 0], proj_in.at[p], p_send.at[0, 0], p_recv.at[p], sibling).wait_recv()

    projected = jnp.sum(proj_in[...], axis=0)
    sensed = jnp.sum(sens_in[...], axis=0)
    out[...] = jnp.sum(projected * sensed, axis=0, keepdims=True)

    for d in range(1, n):
        x_copy(d).wait_send()
        for dq in range(nq):
            spread(d, dq).wait_send()
        for dq in range(1, nq):
            relay(d, dq).wait_send()
    for k in range(1, planes):
        for copy in factor_copies(k):
            copy.wait_send()
        sens_copy(k).wait_send()

    @pl.when(jnp.logical_not(is_end))
    def _():
        stat_copy.wait_send()

    @pl.when(z > 0)
    def _():
        @pl.loop(0, chunks)
        def _(c):
            down_copy(c).wait_send()

    @pl.when(z < n - 1)
    def _():
        @pl.loop(0, chunks)
        def _(c):
            up_copy(c).wait_send()

    @pl.when(is_end)
    def _():
        for s in range(half):
            for k in range(planes):
                if k > 0:
                    proj_copy(s, k).wait_send()
                else:
                    @pl.when(slot != s)
                    def _():
                        proj_copy(s, k).wait_send()


def in_one_kernel(n, nq, nm, residual, norm_gain, gate_weight, up_weight, out_grad, left_factor, right_factor):
    rows, features = residual.shape
    depth, cols = gate_weight.shape
    width = out_grad.shape[1]
    rank = left_factor.shape[1]
    planes = nq * nm
    chunks, half = cols // LANES, n // 2
    bf16, f32 = jnp.bfloat16, jnp.float32
    dma = pltpu.SemaphoreType.DMA
    return pl.pallas_call(
        functools.partial(kernel, n, nq, nm),
        out_shape=jax.ShapeDtypeStruct((1, rows), f32),
        in_specs=[pl.BlockSpec(memory_space=pl.ANY)] * 7,
        out_specs=pl.BlockSpec(memory_space=pltpu.VMEM),
        scratch_shapes=[
            pltpu.VMEM((n * rows, depth), bf16),
            pltpu.VMEM((n * rows, depth), bf16),
            pltpu.VMEM((chunks, depth, 2 * LANES), bf16),
            pltpu.VMEM((rows, features), bf16),
            pltpu.VMEM((1, features), f32),
            pltpu.VMEM((rows, LANES), f32),
            pltpu.VMEM((half * rows, LANES), f32),
            pltpu.VMEM((chunks, n * rows, 2 * LANES), bf16),
            pltpu.VMEM((chunks, half * rows, 2 * LANES), bf16),
            pltpu.VMEM((chunks, half * rows, 2 * LANES), bf16),
            pltpu.VMEM((planes * rank, cols), bf16),
            pltpu.VMEM((planes * rank, width), bf16),
            pltpu.VMEM((rows, width), bf16),
            pltpu.VMEM((half * rows, cols), bf16),
            pltpu.VMEM((planes, rank, rows), f32),
            pltpu.VMEM((planes, rank, rows), f32),
            pltpu.VMEM((half, planes, rank, rows), f32),
            pltpu.VMEM((planes, rank, rows), f32),
            dma((6,)), dma((chunks, 2)), dma((n,)), dma((n,)),
            dma((n, nq)), dma((n, nq)), dma((n, nq)), dma((n, nq)),
            dma((planes,)), dma((planes,)), dma((planes,)), dma((planes,)),
            dma((planes,)), dma((planes,)), dma((half, planes)), dma((planes,)),
            dma((1,)), dma((half,)),
            dma((chunks,)), dma((chunks,)), dma((chunks,)), dma((chunks,)),
        ],
        compiler_params=pltpu.CompilerParams(has_side_effects=True, vmem_limit_bytes=60 * 2**20),
    )(
        residual, norm_gain[None, :], gate_weight, up_weight, out_grad,
        left_factor.reshape(rank, -1), right_factor.reshape(rank, -1),
    )


def fits(n, nq, nm, residual, gate_weight, out_grad, left_factor):
    rows = residual.shape[0]
    return (
        n % 2 == 0
        and nm == 2
        and rows % LANES == 0
        and rows % (nq * nm * SUBLANES) == 0
        and gate_weight.shape[0] % LANES == 0
        and gate_weight.shape[1] % LANES == 0
        and out_grad.shape[1] % LANES == 0
        and left_factor.shape[0] == 1
        and left_factor.shape[1] % SUBLANES == 0
    )


def solution(mesh):
    placed = (
        P("train", None),
        P(),
        P("train", ("query", "mp")),
        P("train", ("query", "mp")),
        P("train", ("query", "mp")),
        P(("query", "mp"), None, None),
        P(("query", "mp"), None, None),
    )
    n, nq, nm = (mesh.shape[axis] for axis in ("train", "query", "mp"))

    def chosen(residual, norm_gain, gate_weight, up_weight, out_grad, left_factor, right_factor):
        args = (residual, norm_gain, gate_weight, up_weight, out_grad, left_factor, right_factor)
        if fits(n, nq, nm, residual, gate_weight, out_grad, left_factor):
            return in_one_kernel(n, nq, nm, *args)
        return on_device(*args)

    return jax.shard_map(
        chosen,
        mesh=mesh,
        in_specs=placed,
        out_specs=P(("query", "mp"), "train"),
        check_vma=False,
    )
```

```python
import functools

import jax
import jax.numpy as jnp
from jax import lax
from jax.experimental import pallas as pl
from jax.experimental.pallas import tpu as pltpu
from jax.sharding import PartitionSpec as P

norm_eps = 1e-05


def on_device(residual, norm_gain, gate_weight, up_weight, out_grad, left_factor, right_factor):
    values = residual.astype(jnp.float32)
    mean_sq = jnp.mean(values * values, axis=1, keepdims=True)
    normed = (values * lax.rsqrt(mean_sq + norm_eps) * norm_gain[None, :]).astype(jnp.bfloat16)
    tok_rows = normed.shape[0]
    hidden_cols = gate_weight.shape[1]
    all_rows = lax.all_to_all(normed, "train", split_axis=1, concat_axis=0, tiled=True)
    paired = jnp.concatenate([gate_weight, up_weight], axis=1)
    summed = lax.psum_scatter(
        jnp.dot(all_rows, paired, preferred_element_type=jnp.float32).astype(jnp.bfloat16),
        "train",
        scatter_dimension=0,
        tiled=True,
    ).astype(jnp.float32)
    activation = (jax.nn.silu(summed[:, :hidden_cols]) * summed[:, hidden_cols:]).astype(
        jnp.bfloat16
    )
    queries = left_factor.shape[0]
    factor_rank = left_factor.shape[1]
    contract = (((1,), (1,)), ((), ()))
    left_flat = left_factor.reshape(queries * factor_rank, left_factor.shape[2])
    columns = left_flat
    projected = lax.dot_general(
        columns,
        lax.all_gather(activation, ("query", "mp"), axis=1, tiled=True),
        contract,
        preferred_element_type=jnp.float32,
    )
    right_flat = right_factor.reshape(queries * factor_rank, right_factor.shape[2])
    columns = right_flat
    sensed = lax.dot_general(
        columns,
        lax.all_gather(out_grad, ("query", "mp"), axis=1, tiled=True),
        contract,
        preferred_element_type=jnp.float32,
    )
    return jnp.sum((projected * sensed).reshape(queries, factor_rank, tok_rows), axis=1)


LANES = 128
SUBLANES = 16
LAG = 2
MESH = pl.DeviceIdType.MESH
NT = (((1,), (1,)), ((), ()))


def remote(src, dst, send_sem, recv_sem, device):
    return pltpu.make_async_remote_copy(
        src_ref=src,
        dst_ref=dst,
        send_sem=send_sem,
        recv_sem=recv_sem,
        device_id=device,
        device_id_type=MESH,
    )


def kernel(
    n, nq, nm,
    residual, gain, gate, up, grad, left, right,
    out,
    raw, x, w, own, gain_v, stat_own, stat, part, from_up, from_down, lf, rf, grad_v, act,
    sens_part, sens_in, proj_part, proj_in,
    ld_sem, w_sem, x_send, x_recv, f_send, f_recv, sib_send, sib_recv,
    l_send, l_recv, r_send, r_recv, s_send, s_recv, p_send, p_recv, t_send, t_recv,
    dn_send, dn_recv, up_send, up_recv,
):
    q, z, m = lax.axis_index("query"), lax.axis_index("train"), lax.axis_index("mp")
    planes = nq * nm
    p = q * nm + m
    rows = residual.shape[0]
    depth = gate.shape[0]
    cols = gate.shape[1]
    width = grad.shape[1]
    rank = left.shape[0]
    chunks = cols // LANES
    part_rows = rows // planes
    half = n // 2
    side = half * rows
    low = z < half
    end = jnp.where(low, 0, n - 1)
    slot = z - jnp.where(low, 0, half)
    is_end = jnp.logical_or(z == 0, z == n - 1)

    def dev(qq, zz, mm):
        return {"query": qq, "train": zz, "mp": mm}

    sibling = dev(q, z, 1 - m)
    base, other = jnp.where(low, 0, half), jnp.where(low, half, 0)
    barrier = pltpu.get_barrier_semaphore()

    def greet(device):
        pl.semaphore_signal(barrier, inc=1, device_id=device, device_id_type=MESH)

    for s in range(half):
        greet(dev(q, other + s, m))
        for k in range(planes):
            to = lax.rem(p + k, planes)
            if k > 0:
                greet(dev(to // nm, base + s, lax.rem(to, nm)))
            else:
                @pl.when(slot != s)
                def _():
                    greet(dev(q, base + s, m))

    def piece(zz, qq, mm):
        start = zz * rows + (qq * nm + mm) * part_rows
        return raw.at[pl.ds(pl.multiple_of(start, part_rows), part_rows), :]

    def around(d):
        return lax.rem(z + d, n)

    def x_copy(d):
        zt = around(d)
        return remote(
            residual.at[
                pl.ds(pl.multiple_of(p * part_rows, part_rows), part_rows),
                pl.ds(pl.multiple_of(zt * depth, depth), depth),
            ],
            piece(z, q, m), x_send.at[d], x_recv.at[z], dev(q, zt, m),
        )

    own_x = pltpu.make_async_copy(
        residual.at[:, pl.ds(pl.multiple_of(z * depth, depth), depth)],
        raw.at[pl.ds(pl.multiple_of(z * rows, rows), rows), :], ld_sem.at[0])
    own_all = pltpu.make_async_copy(residual, own, ld_sem.at[1])
    gain_copy = pltpu.make_async_copy(gain, gain_v, ld_sem.at[2])
    grad_copy = pltpu.make_async_copy(grad, grad_v, ld_sem.at[3])

    def slice_of(factor, span, to):
        return factor.at[:, pl.ds(pl.multiple_of(to * span, LANES), span)]

    def rows_of(ref, who):
        return ref.at[pl.ds(pl.multiple_of(who * rank, rank), rank), :]

    own_l = pltpu.make_async_copy(slice_of(left, cols, p), rows_of(lf, p), ld_sem.at[4])
    own_r = pltpu.make_async_copy(slice_of(right, width, p), rows_of(rf, p), ld_sem.at[5])
    for copy in (own_all, own_x, gain_copy):
        copy.start()
    pl.semaphore_wait(barrier, half * planes - 1 + half)
    for d in range(1, n):
        x_copy(d).start()
    for copy in (grad_copy, own_r, own_l):
        copy.start()

    def w_copies(c):
        at = pl.ds(pl.multiple_of(c * LANES, LANES), LANES)
        return (
            pltpu.make_async_copy(gate.at[:, at], w.at[c, :, pl.ds(0, LANES)], w_sem.at[c, 0]),
            pltpu.make_async_copy(up.at[:, at], w.at[c, :, pl.ds(LANES, LANES)], w_sem.at[c, 1]),
        )

    @pl.loop(0, chunks)
    def _(c):
        for copy in w_copies(c):
            copy.start()

    own_all.wait()

    @pl.loop(0, rows // SUBLANES)
    def _(i):
        at = pl.ds(pl.multiple_of(i * SUBLANES, SUBLANES), SUBLANES)
        v = own[at, :].astype(jnp.float32)
        mean_sq = jnp.mean(v * v, axis=1, keepdims=True)
        stat_own[at, :] = jnp.broadcast_to(lax.rsqrt(mean_sq + norm_eps), (SUBLANES, LANES))

    def stat_rows(s):
        return pl.ds(pl.multiple_of(s * rows, rows), rows)

    stat_copy = remote(
        stat_own, stat.at[stat_rows(slot), :], t_send.at[0], t_recv.at[slot], dev(q, end, m))

    @pl.when(is_end)
    def _():
        stat[stat_rows(slot), :] = stat_own[...]

    @pl.when(jnp.logical_not(is_end))
    def _():
        stat_copy.start()

    def spread(d, dq):
        zs = around(d)
        if dq == 0:
            return remote(piece(zs, q, m), piece(zs, q, m), sib_send.at[d, 0], sib_recv.at[zs, q], sibling)
        return remote(
            piece(zs, q, m), piece(zs, q, m), f_send.at[d, dq], f_recv.at[zs, q],
            dev(lax.rem(q + dq, nq), z, m))

    def relay(d, dq):
        zs, qs = around(d), lax.rem(q + dq, nq)
        return remote(
            piece(zs, qs, m), piece(zs, qs, m), sib_send.at[d, dq], sib_recv.at[zs, qs], sibling)

    for d in range(1, n):
        zs = around(d)
        remote(piece(zs, q, m), piece(zs, q, m), x_send.at[d], x_recv.at[zs], sibling).wait_recv()
        for dq in range(nq):
            spread(d, (dq + 1) % nq).start()

    def factor_copy(k, which):
        to = lax.rem(p + k, planes)
        device = dev(to // nm, z, lax.rem(to, nm))
        if which == 0:
            return remote(slice_of(right, width, to), rows_of(rf, p), r_send.at[k], r_recv.at[p], device)
        return remote(slice_of(left, cols, to), rows_of(lf, p), l_send.at[k], l_recv.at[p], device)

    for d in range(1, n):
        zs = around(d)
        for dq in range(1, nq):
            qs = lax.rem(q + dq, nq)
            remote(piece(zs, qs, m), piece(zs, qs, m), f_send.at[d, dq], f_recv.at[zs, qs], sibling).wait_recv()
            relay(d, dq).start()
    for which in range(2):
        for k in range(1, planes):
            factor_copy(k, which).start()
    own_x.wait()
    gain_copy.wait()
    for d in range(1, n):
        zs = around(d)
        for dq in range(nq):
            qs = lax.rem(q + dq, nq)
            at = piece(zs, qs, 1 - m)
            remote(at, at, sib_send.at[d, dq], sib_recv.at[zs, qs], sibling).wait_recv()

    @pl.loop(0, n * rows // (4 * SUBLANES))
    def _(i):
        at = pl.ds(pl.multiple_of(i * 4 * SUBLANES, 4 * SUBLANES), 4 * SUBLANES)
        g = gain_v[:, pl.ds(pl.multiple_of(z * depth, depth), depth)]
        x[at, :] = (raw[at, :].astype(jnp.float32) * g).astype(jnp.bfloat16)

    down_rows, up_rows = pl.ds(0, side), pl.ds(side, side)

    def down_copy(c):
        return remote(
            part.at[c, down_rows, :], from_up.at[c], dn_send.at[c], dn_recv.at[c],
            dev(q, jnp.maximum(z - 1, 0), m))

    def up_copy(c):
        return remote(
            part.at[c, up_rows, :], from_down.at[c], up_send.at[c], up_recv.at[c],
            dev(q, jnp.minimum(z + 1, n - 1), m))

    for s in range(half):
        arrives = jnp.logical_and(is_end, slot != s)

        @pl.when(arrives)
        def _():
            remote(stat_own, stat.at[stat_rows(s), :], t_send.at[0], t_recv.at[s], sibling).wait_recv()

    def finish(c, total):
        s = stat[:, 0:1]
        g = total[:, :LANES] * s
        u = total[:, LANES:] * s
        act[:, pl.ds(pl.multiple_of(c * LANES, LANES), LANES)] = (
            g / (1.0 + jnp.exp(-g)) * u).astype(jnp.bfloat16)

    def pass_on(i, hops, arrived, copy, keep, last):
        c = i - LAG * hops

        @pl.when(jnp.logical_and(hops > 0, jnp.logical_and(c >= 0, c < chunks)))
        def _():
            copy(c).wait_recv()

            @pl.when(last)
            def _():
                finish(c, part[c, keep, :].astype(jnp.float32) + arrived[c].astype(jnp.float32))

            @pl.when(jnp.logical_not(last))
            def _():
                part[c, keep, :] = (
                    part[c, keep, :].astype(jnp.float32) + arrived[c].astype(jnp.float32)
                ).astype(jnp.bfloat16)
                copy(c).start()

    def sens_copy(k):
        to = lax.rem(p + k, planes)
        return remote(
            sens_part.at[to], sens_in.at[p], s_send.at[k], s_recv.at[p],
            dev(to // nm, z, lax.rem(to, nm)))

    def step(i, carry):
        @pl.when(i < chunks)
        def _():
            for copy in w_copies(i):
                copy.wait()
            part[i] = jnp.dot(x[...], w[i], preferred_element_type=jnp.float32).astype(jnp.bfloat16)

            @pl.when(z == n - 1)
            def _():
                down_copy(i).start()

            @pl.when(z == 0)
            def _():
                up_copy(i).start()

        pass_on(i, n - 1 - z, from_up, down_copy, down_rows, z == 0)
        pass_on(i, z, from_down, up_copy, up_rows, z == n - 1)

        @pl.when(i == chunks)
        def _():
            own_r.wait()
            grad_copy.wait()
            for k in range(1, planes):
                who = lax.rem(p + k, planes)
                at = rows_of(rf, who)
                remote(at, at, r_send.at[k], r_recv.at[who], sibling).wait_recv()
            sens_part[...] = lax.dot_general(
                rf[...], grad_v[...], NT, preferred_element_type=jnp.float32
            ).reshape(planes, rank, rows)
            sens_in[p] = sens_part[p]
            for k in range(1, planes):
                sens_copy(k).start()

        return carry

    lax.fori_loop(0, chunks + LAG * (n - 1), step, 0)

    own_l.wait()
    for k in range(1, planes):
        who = lax.rem(p + k, planes)
        at = rows_of(lf, who)
        remote(at, at, l_send.at[k], l_recv.at[who], sibling).wait_recv()

    def proj_copy(s, k):
        to = lax.rem(p + k, planes)
        return remote(
            proj_part.at[s, to], proj_in.at[p], p_send.at[s, k], p_recv.at[p],
            dev(to // nm, jnp.where(low, 0, half) + s, lax.rem(to, nm)))

    @pl.when(is_end)
    def _():
        product = lax.dot_general(lf[...], act[...], NT, preferred_element_type=jnp.float32)
        for s in range(half):
            proj_part[s] = product[:, s * rows:(s + 1) * rows].reshape(planes, rank, rows)
        for s in range(half):
            for k in range(planes):
                if k > 0:
                    proj_copy(s, k).start()
                else:
                    @pl.when(slot == s)
                    def _():
                        proj_in[p] = proj_part[s, p]

                    @pl.when(slot != s)
                    def _():
                        proj_copy(s, k).start()

    for k in range(1, planes):
        who = lax.rem(p + k, planes)
        remote(sens_part.at[0], sens_in.at[who], s_send.at[k], s_recv.at[who], sibling).wait_recv()
    for k in range(1, planes):
        who = lax.rem(p + k, planes)
        remote(proj_part.at[0, 0], proj_in.at[who], p_send.at[0, k], p_recv.at[who], sibling).wait_recv()

    @pl.when(jnp.logical_not(is_end))
    def _():
        remote(proj_part.at[0, 0], proj_in.at[p], p_send.at[0, 0], p_recv.at[p], sibling).wait_recv()

    projected = jnp.sum(proj_in[...], axis=0)
    sensed = jnp.sum(sens_in[...], axis=0)
    out[...] = jnp.sum(projected * sensed, axis=0, keepdims=True)

    for d in range(1, n):
        x_copy(d).wait_send()
        for dq in range(nq):
            spread(d, dq).wait_send()
        for dq in range(1, nq):
            relay(d, dq).wait_send()
    for k in range(1, planes):
        for which in range(2):
            factor_copy(k, which).wait_send()
        sens_copy(k).wait_send()

    @pl.when(jnp.logical_not(is_end))
    def _():
        stat_copy.wait_send()

    @pl.when(z > 0)
    def _():
        @pl.loop(0, chunks)
        def _(c):
            down_copy(c).wait_send()

    @pl.when(z < n - 1)
    def _():
        @pl.loop(0, chunks)
        def _(c):
            up_copy(c).wait_send()

    @pl.when(is_end)
    def _():
        for s in range(half):
            for k in range(planes):
                if k > 0:
                    proj_copy(s, k).wait_send()
                else:
                    @pl.when(slot != s)
                    def _():
                        proj_copy(s, k).wait_send()


def in_one_kernel(n, nq, nm, residual, norm_gain, gate_weight, up_weight, out_grad, left_factor, right_factor):
    rows, features = residual.shape
    depth, cols = gate_weight.shape
    width = out_grad.shape[1]
    rank = left_factor.shape[1]
    planes = nq * nm
    chunks, half = cols // LANES, n // 2
    bf16, f32 = jnp.bfloat16, jnp.float32
    dma = pltpu.SemaphoreType.DMA
    return pl.pallas_call(
        functools.partial(kernel, n, nq, nm),
        out_shape=jax.ShapeDtypeStruct((1, rows), f32),
        in_specs=[pl.BlockSpec(memory_space=pl.ANY)] * 7,
        out_specs=pl.BlockSpec(memory_space=pltpu.VMEM),
        scratch_shapes=[
            pltpu.VMEM((n * rows, depth), bf16),
            pltpu.VMEM((n * rows, depth), bf16),
            pltpu.VMEM((chunks, depth, 2 * LANES), bf16),
            pltpu.VMEM((rows, features), bf16),
            pltpu.VMEM((1, features), f32),
            pltpu.VMEM((rows, LANES), f32),
            pltpu.VMEM((half * rows, LANES), f32),
            pltpu.VMEM((chunks, n * rows, 2 * LANES), bf16),
            pltpu.VMEM((chunks, half * rows, 2 * LANES), bf16),
            pltpu.VMEM((chunks, half * rows, 2 * LANES), bf16),
            pltpu.VMEM((planes * rank, cols), bf16),
            pltpu.VMEM((planes * rank, width), bf16),
            pltpu.VMEM((rows, width), bf16),
            pltpu.VMEM((half * rows, cols), bf16),
            pltpu.VMEM((planes, rank, rows), f32),
            pltpu.VMEM((planes, rank, rows), f32),
            pltpu.VMEM((half, planes, rank, rows), f32),
            pltpu.VMEM((planes, rank, rows), f32),
            dma((6,)), dma((chunks, 2)), dma((n,)), dma((n,)),
            dma((n, nq)), dma((n, nq)), dma((n, nq)), dma((n, nq)),
            dma((planes,)), dma((planes,)), dma((planes,)), dma((planes,)),
            dma((planes,)), dma((planes,)), dma((half, planes)), dma((planes,)),
            dma((1,)), dma((half,)),
            dma((chunks,)), dma((chunks,)), dma((chunks,)), dma((chunks,)),
        ],
        compiler_params=pltpu.CompilerParams(collective_id=0, has_side_effects=True, vmem_limit_bytes=60 * 2**20),
    )(
        residual, norm_gain[None, :], gate_weight, up_weight, out_grad,
        left_factor.reshape(rank, -1), right_factor.reshape(rank, -1),
    )


def fits(n, nq, nm, residual, gate_weight, out_grad, left_factor):
    rows = residual.shape[0]
    return (
        n % 2 == 0
        and nm == 2
        and rows % LANES == 0
        and rows % (nq * nm * SUBLANES) == 0
        and gate_weight.shape[0] % LANES == 0
        and gate_weight.shape[1] % LANES == 0
        and out_grad.shape[1] % LANES == 0
        and left_factor.shape[0] == 1
        and left_factor.shape[1] % SUBLANES == 0
    )


def solution(mesh):
    placed = (
        P("train", None),
        P(),
        P("train", ("query", "mp")),
        P("train", ("query", "mp")),
        P("train", ("query", "mp")),
        P(("query", "mp"), None, None),
        P(("query", "mp"), None, None),
    )
    n, nq, nm = (mesh.shape[axis] for axis in ("train", "query", "mp"))

    def chosen(residual, norm_gain, gate_weight, up_weight, out_grad, left_factor, right_factor):
        args = (residual, norm_gain, gate_weight, up_weight, out_grad, left_factor, right_factor)
        if fits(n, nq, nm, residual, gate_weight, out_grad, left_factor):
            return in_one_kernel(n, nq, nm, *args)
        return on_device(*args)

    return jax.shard_map(
        chosen,
        mesh=mesh,
        in_specs=placed,
        out_specs=P(("query", "mp"), "train"),
        check_vma=False,
    )
```
